8 devices in a mesh: dp: 4 (over z, y, x), tp: 2 (over core).
Axes of the slice: x: 2, y: 2, z: 1, core: 2. Of those that a mesh axis runs over, the one named last changes fastest.
Arguments:
- x_stored: bfloat16 [3, 64, 256, 1600], P(None, 'dp')
- u_stored: bfloat16 [3, 64, 256, 6400], P(None, 'dp', None, 'tp')
- w_up: bfloat16 [3, 1600, 6400], P(None, None, 'tp')
- w_down: bfloat16 [3, 6400, 1600], P(None, 'tp')
- d_out: bfloat16 [64, 256, 1600], P('dp')
- noise_up: float32 [3, 1600, 6400], P(None, 'dp', 'tp')
- noise_down: float32 [3, 6400, 1600], P(None, 'tp', 'dp')
- clip_up: float32 [3], replicated
- clip_down: float32 [3], replicated
- noise_mult: float32 [1], replicated
Outputs:
- output 1: float32 [3, 1600, 6400], P(None, 'dp', 'tp')
- output 2: float32 [3, 6400, 1600], P(None, 'tp', 'dp')
All inputs are finite; a program needn't handle non-finite values.
Results may differ from the reference program's by a relative error of at most 0.0112699.
Values are sent between devices in bfloat16 or wider.
A program may use at most 1 GiB of HBM per device.

```python
import math
import jax
import jax.numpy as jnp
from jax import lax

NUM_LAYERS = 3
NUM_EXAMPLES = 64
SEQ_LEN = 256
D_MODEL = 1600
D_FF = 6400

GELU_SCALE = math.sqrt(2.0 / math.pi)


def gelu_pair(pre_act):
    tanh_val = jnp.tanh(GELU_SCALE * (pre_act + 0.044715 * pre_act * pre_act * pre_act))
    gelu_val = 0.5 * pre_act * (1.0 + tanh_val)
    gelu_slope = 0.5 * (1.0 + tanh_val) + 0.5 * pre_act * (1.0 - tanh_val * tanh_val) * GELU_SCALE * (1.0 + 0.134145 * pre_act * pre_act)
    return gelu_val, gelu_slope


def setup_inputs(seed: int = 0) -> dict:
    key_list = jax.random.split(jax.random.key(seed), 11)
    x_stored = jax.random.normal(key_list[0], (NUM_LAYERS, NUM_EXAMPLES, SEQ_LEN, D_MODEL), jnp.float32).astype(jnp.bfloat16)
    u_stored = jax.random.normal(key_list[1], (NUM_LAYERS, NUM_EXAMPLES, SEQ_LEN, D_FF), jnp.float32).astype(jnp.bfloat16)
    w_up = (jax.random.normal(key_list[2], (NUM_LAYERS, D_MODEL, D_FF), jnp.float32) * D_MODEL ** -0.5).astype(jnp.bfloat16)
    w_down = (jax.random.normal(key_list[3], (NUM_LAYERS, D_FF, D_MODEL), jnp.float32) * D_FF ** -0.5).astype(jnp.bfloat16)
    row_scale = 2.0 ** jax.random.uniform(key_list[4], (NUM_EXAMPLES, 1, 1), jnp.float32, minval=-1.5, maxval=1.5)
    d_out = (jax.random.normal(key_list[5], (NUM_EXAMPLES, SEQ_LEN, D_MODEL), jnp.float32) * row_scale).astype(jnp.bfloat16)
    noise_up = jax.random.normal(key_list[6], (NUM_LAYERS, D_MODEL, D_FF), jnp.float32)
    noise_down = jax.random.normal(key_list[7], (NUM_LAYERS, D_FF, D_MODEL), jnp.float32)
    depth_pow = jnp.arange(NUM_LAYERS - 1, -1, -1).astype(jnp.float32)
    typical = math.sqrt(SEQ_LEN * D_MODEL * D_FF) * 1.2 ** depth_pow
    clip_up = typical * 0.335 * jax.random.uniform(key_list[8], (NUM_LAYERS,), jnp.float32, minval=0.2, maxval=0.5)
    clip_down = typical * 0.63 * jax.random.uniform(key_list[9], (NUM_LAYERS,), jnp.float32, minval=0.2, maxval=0.5)
    noise_mult = jax.random.uniform(key_list[10], (1,), jnp.float32, minval=0.25, maxval=0.6) * math.sqrt(NUM_EXAMPLES / (D_MODEL * D_FF))
    return {"x_stored": x_stored, "u_stored": u_stored, "w_up": w_up, "w_down": w_down, "d_out": d_out, "noise_up": noise_up, "noise_down": noise_down, "clip_up": clip_up, "clip_down": clip_down, "noise_mult": noise_mult}


def example_norms(x_layer, hidden, grad_z, grad_h):
    def one_example(example):
        x_row, h_row, dz_row, dh_row = example
        gram_x = jnp.dot(x_row, x_row.T, preferred_element_type=jnp.float32)
        gram_dh = jnp.dot(dh_row, dh_row.T, preferred_element_type=jnp.float32)
        gram_h = jnp.dot(h_row, h_row.T, preferred_element_type=jnp.float32)
        gram_dz = jnp.dot(dz_row, dz_row.T, preferred_element_type=jnp.float32)
        return jnp.stack([jnp.sum(gram_x * gram_dh), jnp.sum(gram_h * gram_dz)])
    return lax.map(one_example, (x_layer, hidden, grad_z, grad_h))


def reference(x_stored, u_stored, w_up, w_down, d_out, noise_up, noise_down, clip_up, clip_down, noise_mult):
    def layer_step(grad_z, layer_in):
        x_layer, u_layer, up_w, down_w, up_noise, down_noise, up_clip, down_clip = layer_in
        gelu_val, gelu_slope = gelu_pair(u_layer.astype(jnp.float32))
        hidden = gelu_val.astype(jnp.bfloat16)
        back_h = jnp.dot(grad_z.reshape(-1, D_MODEL), down_w.T, preferred_element_type=jnp.float32)
        grad_h = (gelu_slope * back_h.reshape(u_layer.shape)).astype(jnp.bfloat16)
        back_x = jnp.dot(grad_h.reshape(-1, D_FF), up_w.T, preferred_element_type=jnp.float32)
        next_z = (grad_z.astype(jnp.float32) + back_x.reshape(grad_z.shape)).astype(jnp.bfloat16)
        ghost_norms = example_norms(x_layer, hidden, grad_z, grad_h)
        scale_up = jnp.minimum(1.0, up_clip / jnp.sqrt(ghost_norms[:, 0]))
        scale_down = jnp.minimum(1.0, down_clip / jnp.sqrt(ghost_norms[:, 1]))
        dh_clip = (grad_h.astype(jnp.float32) * scale_up[:, None, None]).astype(jnp.bfloat16)
        dz_clip = (grad_z.astype(jnp.float32) * scale_down[:, None, None]).astype(jnp.bfloat16)
        sum_up = jnp.dot(x_layer.reshape(-1, D_MODEL).T, dh_clip.reshape(-1, D_FF), preferred_element_type=jnp.float32)
        sum_down = jnp.dot(hidden.reshape(-1, D_FF).T, dz_clip.reshape(-1, D_MODEL), preferred_element_type=jnp.float32)
        grad_up = (sum_up + noise_mult[0] * up_clip * up_noise) / NUM_EXAMPLES
        grad_down = (sum_down + noise_mult[0] * down_clip * down_noise) / NUM_EXAMPLES
        return next_z, (grad_up, grad_down)
    layer_inputs = (x_stored, u_stored, w_up, w_down, noise_up, noise_down, clip_up, clip_down)
    last_z, (grads_up, grads_down) = lax.scan(layer_step, d_out, layer_inputs, reverse=True)
    return grads_up, grads_down
```

```python
import math
import jax
import jax.numpy as jnp
from jax import lax
from jax.sharding import PartitionSpec as P

GELU_SCALE = math.sqrt(2.0 / math.pi)
BF = jnp.bfloat16
F32 = jnp.float32


def gelu_pair(pre_act):
    tanh_val = jnp.tanh(GELU_SCALE * (pre_act + 0.044715 * pre_act * pre_act * pre_act))
    gelu_val = 0.5 * pre_act * (1.0 + tanh_val)
    gelu_slope = 0.5 * (1.0 + tanh_val) + 0.5 * pre_act * (1.0 - tanh_val * tanh_val) * GELU_SCALE * (1.0 + 0.134145 * pre_act * pre_act)
    return gelu_val, gelu_slope


def gram(a):
    return jnp.einsum("btf,bsf->bts", a, a, preferred_element_type=F32)


def solution(mesh):
    data_size = mesh.shape["dp"]
    in_specs = (P(None, "dp", None, None), P(None, "dp", None, "tp"), P(None, None, "tp"), P(None, "tp", None), P("dp", None, None), P(None, "dp", "tp"), P(None, "tp", "dp"), P(), P(), P())
    out_specs = (P(None, "dp", "tp"), P(None, "tp", "dp"))
    swap_x = [(i, i ^ 1) for i in range(4)]
    swap_y = [(i, i ^ 2) for i in range(4)]
    swap_t = [(0, 1), (1, 0)]

    def local_step(x_stored, u_stored, w_up, w_down, d_out, noise_up, noise_down, clip_up, clip_down, noise_mult):
        num_layers = x_stored.shape[0]
        total_examples = d_out.shape[0] * data_size
        d_model = d_out.shape[2]
        d_blk = d_model // 4
        me = lax.axis_index("dp")
        my_y, my_x = me // 2, me % 2

        order = [None]

        def after(*vals):
            if order[0] is None:
                return vals
            return lax.optimization_barrier((*vals, order[0]))[:-1]

        def cut_rows(src, y, x, num_y, num_x):
            stack, at = src
            view = stack.reshape(*stack.shape[:3], 2, 2, d_blk)
            size = (1, *stack.shape[1:3], num_y, num_x, d_blk)
            return lax.dynamic_slice(view, (at, 0, 0, y, x, 0), size).reshape(*stack.shape[1:3], -1)

        def pick(src, y, x):
            return cut_rows(src, y, x, 1, 1)

        def product(lhs, rhs):
            return jnp.einsum("btd,btf->df", lhs, rhs, preferred_element_type=F32)

        def phase_one(lhs, rhs, cut):
            send_a = cut_rows(lhs, 0, 1 - my_x, 2, 1)
            send_b = cut_rows(lhs, 1 - my_y, 0, 1, 2)
            part_a = product(send_a, rhs[:, :, :cut])
            order[0] = part_a
            got_a = lax.ppermute(part_a, "dp", swap_x)
            send_b, = after(send_b)
            part_b = product(send_b, rhs[:, :, cut:])
            order[0] = part_b
            got_b = lax.ppermute(part_b, "dp", swap_y)
            return got_a.reshape(2, d_blk, -1), got_b.reshape(2, d_blk, -1)

        def own(lhs, rhs):
            lhs = (*after(lhs[0]), lhs[1])
            res = product(pick(lhs, my_y, my_x), rhs)
            order[0] = res
            return res

        def phase_two(lhs, rhs, cut, got_a, got_b):
            whole, got_a, got_b = after(lhs[0], got_a, got_b)
            lhs = (whole, lhs[1])
            part_a = product(pick(lhs, 1 - my_y, my_x), rhs[:, :, :cut]) + lax.dynamic_index_in_dim(got_a, 1 - my_y, 0, keepdims=False)
            part_b = product(pick(lhs, my_y, 1 - my_x), rhs[:, :, cut:]) + lax.dynamic_index_in_dim(got_b, 1 - my_x, 0, keepdims=False)
            order[0] = part_b
            fin_a = lax.ppermute(part_a, "dp", swap_y)
            fin_b = lax.ppermute(part_b, "dp", swap_x)
            return fin_a, fin_b

        def finish(own_part, got_a, got_b, fin_a, fin_b, noise):
            side_a = fin_a + lax.dynamic_index_in_dim(got_a, my_y, 0, keepdims=False)
            side_b = fin_b + lax.dynamic_index_in_dim(got_b, my_x, 0, keepdims=False)
            return (own_part + jnp.concatenate([side_a, side_b], axis=1) + noise) / total_examples

        def over_tp(v):
            return v + lax.ppermute(v, "tp", swap_t)

        out_up = jnp.zeros(noise_up.shape, F32)
        out_down = jnp.zeros((num_layers, noise_down.shape[2], noise_down.shape[1]), F32)
        noise_down_t = jnp.swapaxes(noise_down, 1, 2)
        grad_z = d_out
        pend = None
        for layer in reversed(range(num_layers)):
            x_layer = (x_stored, layer)
            u_all, = after(u_stored)
            hidden = gelu_pair(u_all[layer].astype(F32))[0].astype(BF)
            norm_down = over_tp(jnp.sum(gram(hidden) * gram(grad_z), axis=(1, 2)))
            order[0] = norm_down
            scale_down = jnp.minimum(1.0, clip_down[layer] / jnp.sqrt(norm_down))
            dz_clip = ((grad_z.astype(F32) * scale_down[:, None, None]).astype(BF)[None], 0)
            cut = 1664
            got_da, got_db = phase_one(dz_clip, hidden, cut)
            if pend is not None:
                pend()
            u_all, = after(u_stored)
            slope = gelu_pair(u_all[layer].astype(F32))[1]
            back_h = jnp.einsum("btd,fd->btf", grad_z, w_down[layer], preferred_element_type=F32)
            grad_h = (slope * back_h).astype(BF)
            order[0] = grad_h
            own_d = own(dz_clip, hidden)
            fin_da, fin_db = phase_two(dz_clip, hidden, cut, got_da, got_db)
            x_all, = after(x_stored)
            norm_up = over_tp(jnp.sum(gram(x_all[layer]) * gram(grad_h), axis=(1, 2)))
            order[0] = norm_up
            scale_up = jnp.minimum(1.0, clip_up[layer] / jnp.sqrt(norm_up))
            dh_clip = (grad_h.astype(F32) * scale_up[:, None, None]).astype(BF)
            got_ua, got_ub = phase_one(x_layer, dh_clip, 1536)
            if layer > 0:
                w_all, = after(w_up)
                part_x = jnp.einsum("btf,df->btd", grad_h, w_all[layer], preferred_element_type=F32).astype(BF)
                order[0] = part_x
                full_x = part_x.astype(F32) + lax.ppermute(part_x, "tp", swap_t).astype(F32)
                next_z = (grad_z.astype(F32) + full_x).astype(BF)
            own_u = own(x_layer, dh_clip)
            store = {}

            def second(x_layer=x_layer, dh_clip=dh_clip, got_ua=got_ua, got_ub=got_ub, store=store):
                store["fin"] = phase_two(x_layer, dh_clip, 1536, got_ua, got_ub)

            def close(layer=layer, own_d=own_d, got_da=got_da, got_db=got_db, fin_da=fin_da, fin_db=fin_db, own_u=own_u, got_ua=got_ua, got_ub=got_ub, store=store):
                noise_d = noise_mult[0] * clip_down[layer] * noise_down_t[layer]
                noise_u = noise_mult[0] * clip_up[layer] * noise_up[layer]
                return (finish(own_u, got_ua, got_ub, *store["fin"], noise_u), finish(own_d, got_da, got_db, fin_da, fin_db, noise_d))

            if layer > 0:
                grad_z = next_z
                pend = second
            else:
                second()
            if layer == num_layers - 1:
                closers = []
            closers.append((layer, close))
        for layer, close in closers:
            g_up, g_down = close()
            out_up = lax.dynamic_update_slice(out_up, g_up[None], (layer, 0, 0))
            out_down = lax.dynamic_update_slice(out_down, g_down[None], (layer, 0, 0))
        return out_up, jnp.swapaxes(out_down, 1, 2)

    return jax.shard_map(local_step, mesh=mesh, in_specs=in_specs, out_specs=out_specs, check_vma=False)
```
